128 devices in a mesh: fsdp: 8 (over x, z_lo), tenant: 8 (over y, z_hi), dp: 2 (over core).
Axes of the slice: x: 4, y: 4, z: 4 (z_hi: 2, z_lo: 2; z = z_hi * 2 + z_lo), core: 2. Of those that a mesh axis runs over, the one named last changes fastest.
Arguments:
- tokens: bfloat16 [6144, 5120], P(('fsdp', 'dp'), 'tenant'), may hold values from -6 to 6
- block_tenant_index: int32 [96], P(('fsdp', 'dp')), may hold values from 0 to 7
- ranks: int32 [8], replicated, may hold values from 16 to 64, as said below
- frozen_up_weight: bfloat16 [5120, 14336], P(('fsdp', 'dp'), 'tenant'), may hold values from -0.078125 to 0.078125
- tenant_down_adapters: bfloat16 [8, 64, 5120], P('tenant'), may hold values from -0.078125 to 0.078125
- tenant_up_adapters: bfloat16 [8, 64, 14336], P('tenant'), may hold values from -0.75 to 0.75
- cotangent: bfloat16 [6144, 14336], P(('fsdp', 'dp'), 'tenant'), may hold values from -6 to 6
Outputs:
- hidden_out: bfloat16 [6144, 14336], P(('fsdp', 'dp'), 'tenant')
- grad_tokens: bfloat16 [6144, 5120], P(('fsdp', 'dp'), 'tenant')
- grad_down: float32 [8, 64, 5120], P('dp', None, 'tenant')
- grad_up: float32 [8, 64, 14336], P('dp', None, 'tenant')
The draws below stay inside these ranges and needn't reach their ends.
Inputs may be any that keep to these rules, and one draw needn't show every extreme that they name: `ranks`: multiples of 16; some tenant has rank 64.
All inputs are finite; a program needn't handle non-finite values.
Results may differ from the reference program's by a relative error of at most 0.0034.
Values may be sent and summed in bfloat16 or wider, within the bound.
No kernel may reach another device: no remote copies, remote signals or barrier semaphores. Data moves between devices by JAX's collectives and lax.ppermute only.
A program may use at most 128 MiB of HBM per device.

```python
import math
import jax
import jax.numpy as jnp
import numpy as np

MODEL_WIDTH = 5120
HIDDEN_UNITS = 14336
TENANT_COUNT = 8
ADAPTER_RANK = 64
BLOCK = 64
TOKENS = 6144
BLOCKS = 96


def draw_ranks(key, part):
    levels = jax.random.randint(key, (TENANT_COUNT,), 1, ADAPTER_RANK // 16 + 1)
    chosen = jax.random.randint(jax.random.fold_in(key, 7), (), 0, TENANT_COUNT)
    levels = jnp.where(jnp.arange(TENANT_COUNT) == chosen, ADAPTER_RANK // 16, levels)
    return (levels * 16).astype(jnp.int32)


def place_ends(drawn, key, least, high):
    place = [jax.random.randint(jax.random.fold_in(key, axis), (), 0, length) for axis, length in enumerate(drawn.shape)]
    main_axis = drawn.shape.index(max(drawn.shape))
    next_to = place[:main_axis] + [(place[main_axis] + 1) % drawn.shape[main_axis]] + place[main_axis + 1:]
    return drawn.at[tuple(place)].set(least).at[tuple(next_to)].set(high)


def shard_levels(key, extent, shards, smallest, top_value):
    factor_of = 1.0
    for dim, blocks in shards:
        steps = jax.random.uniform(jax.random.fold_in(jax.random.fold_in(key, 6), dim), (blocks,), jnp.float32, smallest / len(shards), top_value / len(shards))
        factor_of = factor_of * jnp.repeat(jnp.exp(steps), extent[dim] // blocks).reshape((-1,) + (1,) * (len(extent) - 1 - dim))
    return factor_of


def rank_table(number_of, lean):
    weights = [(1 << 20) // math.isqrt(grade ** lean) + 1 for grade in range(1, number_of + 1)]
    deviation = 1 + sum(weights) // (1 << 30)
    return np.cumsum(np.array([max(1, weight // deviation) for weight in weights]))


def ranked(stream_key, extent, number_of, skew):
    grid = rank_table(number_of, skew)
    pick = jax.random.randint(jax.random.fold_in(stream_key, 1), extent, 0, int(grid[number_of - 1]))
    rank = jnp.searchsorted(jnp.asarray(grid, jnp.int32), pick, side="right")
    return jax.random.permutation(jax.random.fold_in(stream_key, 2), number_of)[rank].astype(jnp.int32)


def centred(stream_key, extent, spread, most, shards=(), kind=jnp.bfloat16):
    result = spread * jax.random.normal(stream_key, extent, jnp.float32)
    if shards:
        result = result * shard_levels(stream_key, extent, shards, -0.22, 0.18)
    return jnp.clip(result, -most, most).astype(kind)


def setup_inputs(seed: int = 0) -> dict:
    splits = jax.random.split(jax.random.key(seed), 8)
    return {
        "tokens": centred(splits[0], (TOKENS, MODEL_WIDTH), 1.0, 6.0, ((0, 16), (1, 8))),
        "block_tenant_index": place_ends(ranked(splits[1], (BLOCKS,), TENANT_COUNT, 2), jax.random.fold_in(splits[1], 3), 0, TENANT_COUNT - 1).astype(jnp.int32),
        "ranks": draw_ranks(jax.random.fold_in(splits[7], 71), 0),
        "frozen_up_weight": centred(splits[3], (MODEL_WIDTH, HIDDEN_UNITS), MODEL_WIDTH ** -0.5, 0.078125, ((0, 16), (1, 8))),
        "tenant_down_adapters": centred(splits[4], (TENANT_COUNT, ADAPTER_RANK, MODEL_WIDTH), MODEL_WIDTH ** -0.5, 0.078125, ((0, 8),)),
        "tenant_up_adapters": centred(splits[5], (TENANT_COUNT, ADAPTER_RANK, HIDDEN_UNITS), ADAPTER_RANK ** -0.5, 0.75, ((0, 8),)),
        "cotangent": centred(splits[6], (TOKENS, HIDDEN_UNITS), 1.0, 6.0, ((0, 16), (1, 8))),
    }


alpha_scale = 32.0


def make_gain(block_tenant_index, ranks):
    rows_tenant = jnp.repeat(block_tenant_index, BLOCK, total_repeat_length=TOKENS)
    columns = jnp.arange(TENANT_COUNT * ADAPTER_RANK, dtype=jnp.int32)
    col_tenant = columns // ADAPTER_RANK
    col_slot = columns % ADAPTER_RANK
    ranks_col = jnp.repeat(ranks, ADAPTER_RANK, total_repeat_length=TENANT_COUNT * ADAPTER_RANK)
    keep = (rows_tenant[:, None] == col_tenant[None, :]) & (col_slot[None, :] < ranks_col[None, :])
    scale_col = alpha_scale / ranks_col.astype(jnp.float32)
    return jnp.where(keep, scale_col[None, :], jnp.float32(0.0))


def reference(tokens, block_tenant_index, ranks, frozen_up_weight, tenant_down_adapters, tenant_up_adapters, cotangent):
    gain = make_gain(block_tenant_index, ranks)
    flattened_down = tenant_down_adapters.reshape(TENANT_COUNT * ADAPTER_RANK, MODEL_WIDTH)
    flattened_up = tenant_up_adapters.reshape(TENANT_COUNT * ADAPTER_RANK, HIDDEN_UNITS)
    proj = jnp.dot(tokens, flattened_down.T, preferred_element_type=jnp.float32)
    adapted = (proj * gain).astype(jnp.bfloat16)
    base = jnp.dot(tokens, frozen_up_weight, preferred_element_type=jnp.float32)
    hidden_out = (base + jnp.dot(adapted, flattened_up, preferred_element_type=jnp.float32)).astype(jnp.bfloat16)
    back = jnp.dot(cotangent, flattened_up.T, preferred_element_type=jnp.float32)
    adapted_grad = (back * gain).astype(jnp.bfloat16)
    grad_base = jnp.dot(cotangent, frozen_up_weight.T, preferred_element_type=jnp.float32)
    grad_tokens = (grad_base + jnp.dot(adapted_grad, flattened_down, preferred_element_type=jnp.float32)).astype(jnp.bfloat16)
    grad_up = jnp.dot(adapted.T, cotangent, preferred_element_type=jnp.float32).reshape(TENANT_COUNT, ADAPTER_RANK, HIDDEN_UNITS)
    grad_down = jnp.dot(adapted_grad.T, tokens, preferred_element_type=jnp.float32).reshape(TENANT_COUNT, ADAPTER_RANK, MODEL_WIDTH)
    return hidden_out, grad_tokens, grad_down, grad_up
```

```python
import jax
import jax.numpy as jnp
from jax import lax
from jax.sharding import PartitionSpec as P

BLOCK = 64
ALPHA = 32.0
F32 = jnp.float32
BF16 = jnp.bfloat16


def ring_pairs(size, step, flip):
    ring = size // 2
    return [(r * 2 + b, ((r + step) % ring) * 2 + (b ^ flip)) for r in range(ring) for b in range(2)]


def move(value, axis, step=0, flip=0):
    return lax.ppermute(value, axis, ring_pairs(lax.axis_size(axis), step, flip))


def swap_cores(value):
    return lax.ppermute(value, "dp", [(0, 1), (1, 0)])


def mirror(value, axis, shift):
    ring = lax.axis_size(axis) // 2
    pairs = []
    for r in range(ring):
        other = ((r - shift) % ring ^ 1) + shift
        for b in range(2):
            pairs.append((r * 2 + b, (other % ring) * 2 + b))
    return lax.ppermute(value, axis, pairs)


def gather_ring(own, axis):
    out = {(0, 0): own}
    out[0, 1] = move(own, axis, 0, 1)
    out[-1, 0] = move(own, axis, 1)
    out[1, 0] = move(own, axis, -1)
    out[2, 0] = move(out[-1, 0], axis, 1)
    out[1, 1] = move(out[0, 1], axis, -1)
    out[-1, 1] = move(out[0, 1], axis, 1)
    out[2, 1] = move(out[1, 1], axis, -1)
    return out


def pick(array, index):
    return lax.dynamic_index_in_dim(array, index, 0, keepdims=False)


def dot(a, b, ca, cb):
    return lax.dot_general(a, b, (((ca,), (cb,)), ((), ())), preferred_element_type=F32)


def in_core_order(mine, other, core, axis=0):
    first = jnp.where(core == 0, mine, other)
    second = jnp.where(core == 0, other, mine)
    return jnp.concatenate([first, second], axis=axis)


def shards(tokens, block_tenant_index, ranks, weight, down, up, cotangent):
    rows, local_d = tokens.shape
    local_f = cotangent.shape[1]
    tenants = ranks.shape[0]
    rank = down.shape[1]
    half = rank // 2
    width = local_f + local_d
    f_at, t_at, core = lax.axis_index("fsdp"), lax.axis_index("tenant"), lax.axis_index("dp")
    x_at, zl_at = f_at // 2, f_at % 2
    y_at, zh_at = t_at // 2, t_at % 2

    w_mine = gather_ring(weight, "fsdp")
    w_other = {k: swap_cores(v) for k, v in w_mine.items()}
    tok_parts = gather_ring(tokens, "tenant")
    tok_all = jnp.zeros((tenants, rows, local_d), BF16)
    for (step, flip), part in tok_parts.items():
        at = (y_at + step) % 4 * 2 + (zh_at ^ flip)
        tok_all = lax.dynamic_update_index_in_dim(tok_all, part, at, 0)

    up_half = lax.dynamic_slice_in_dim(up[0], core * half, half, 0)
    down_half = lax.dynamic_slice_in_dim(down[0], core * half, half, 0)
    blocks = jnp.concatenate(
        [
            jnp.moveaxis(up_half.reshape(half, tenants, local_f), 1, 0),
            jnp.moveaxis(down_half.reshape(half, tenants, local_d), 1, 0),
        ],
        axis=2,
    ).reshape(4, 2, half, width)
    steps = (0, -1, 1, 2)
    by_step = [pick(blocks, y_at)] + [move(pick(blocks, (y_at - s) % 4), "tenant", -s) for s in steps[1:]]
    stacked = jnp.stack(by_step)
    keep = lax.dynamic_index_in_dim(stacked, zh_at, 1, keepdims=False)
    give = lax.dynamic_index_in_dim(stacked, 1 - zh_at, 1, keepdims=False)
    got = jnp.concatenate([keep, move(give, "tenant", 0, 1)])
    adapters = in_core_order(got, swap_cores(got), core, axis=1).reshape(tenants * rank, width)
    up_rows, down_rows = adapters[:, :local_f], adapters[:, local_f:]
    source = jnp.stack([(y_at + s) % 4 * 2 + (zh_at ^ b) for b in (0, 1) for s in steps])
    source_col = jnp.repeat(source, rank, total_repeat_length=tenants * rank)

    rows_tenant = jnp.repeat(block_tenant_index, BLOCK, total_repeat_length=rows)[:, None]
    rows_rank = sum(jnp.where(rows_tenant == s, ranks[s], 0) for s in range(tenants))
    slot = jnp.arange(rank, dtype=jnp.int32)[None, :]
    gain = jnp.where(slot < rows_rank, ALPHA / rows_rank.astype(F32), F32(0.0))

    def own_columns(wide):
        cols = [wide[:, s * rank : (s + 1) * rank] for s in range(tenants)]
        return sum(jnp.where(rows_tenant == source[s], cols[s], F32(0.0)) for s in range(tenants))

    both = jnp.concatenate(
        [own_columns(dot(tokens, down_rows, 1, 1)), own_columns(dot(cotangent, up_rows, 1, 1))], axis=1
    )
    both = both + move(both, "tenant", 0, 1)
    both = both + mirror(both, "tenant", 0)
    both = both + mirror(both, "tenant", 1)
    adapted = (both[:, :rank] * gain).astype(BF16)
    adapted_grad = (both[:, rank:] * gain).astype(BF16)

    def spread(compact, col_tenant):
        return jnp.where(rows_tenant == col_tenant[None, :], jnp.tile(compact, (1, tenants)), BF16(0.0))

    plain_col = jnp.arange(tenants * rank, dtype=jnp.int32) // rank

    up_term = dot(spread(adapted, plain_col), cotangent, 0, 0)
    down_term = dot(spread(adapted_grad, plain_col), tokens, 0, 0)
    term = jnp.concatenate([up_term, down_term], axis=1).reshape(2, tenants * rank // 2, width)
    share = pick(term, core) + swap_cores(pick(term, 1 - core))
    gray = (x_at + 1) // 2 % 2
    late = x_at // 2

    def halve(value, side, send):
        parts = value.reshape(2, value.shape[0] // 2, width)
        return pick(parts, side) + send(pick(parts, 1 - side).astype(BF16)).astype(F32)

    def double(value, side, send):
        other = send(value)
        return jnp.where(side == 0, jnp.concatenate([value, other]), jnp.concatenate([other, value]))

    by_z = lambda v: move(v, "fsdp", 0, 1)
    by_x0 = lambda v: mirror(v, "fsdp", 0)
    by_x1 = lambda v: mirror(v, "fsdp", 1)
    share = halve(share, zl_at, by_z)
    share = halve(share, gray, by_x0)
    share = halve(share, late, by_x1).astype(BF16)
    share = double(share, late, by_x1)
    share = double(share, gray, by_x0)
    share = double(share, zl_at, by_z).astype(F32).reshape(tenants // 2, rank, width)
    grad_up, grad_down = share[:, :, :local_f], share[:, :, local_f:]

    hidden = dot(spread(adapted, source_col), up_rows, 1, 0)
    grads = [jnp.zeros((4, rows, local_d), BF16) for _ in range(2)]
    for (step, flip), mine in w_mine.items():
        block = in_core_order(mine, w_other[step, flip], core)
        x_from = (x_at + step) % 4
        tok = pick(tok_all, x_from * 2 + (zl_at ^ flip))
        hidden = hidden + dot(tok, block, 1, 0)
        part = dot(cotangent, block, 1, 1).astype(BF16)
        grads[flip] = lax.dynamic_update_index_in_dim(grads[flip], part, x_from, 0)
    hidden_out = hidden.astype(BF16)

    def over_ring(parts):
        arrived = [move(pick(parts, (y_at - s) % 4), "tenant", -s) for s in steps[1:]]
        return sum((a.astype(F32) for a in arrived), pick(parts, y_at).astype(F32))

    near, far = over_ring(grads[0]), over_ring(grads[1])
    same = zh_at == zl_at
    given = move(jnp.where(same, far, near).astype(BF16), "tenant", 0, 1)
    kept = jnp.where(same, near, far) + given.astype(F32)
    grad_tokens = (kept + dot(spread(adapted_grad, source_col), down_rows, 1, 0)).astype(BF16)
    return hidden_out, grad_tokens, grad_down, grad_up


def solution(mesh):
    by_rows = P(("fsdp", "dp"), "tenant")
    return jax.shard_map(
        shards,
        mesh=mesh,
        in_specs=(by_rows, P(("fsdp", "dp")), P(), by_rows, P("tenant"), P("tenant"), by_rows),
        out_specs=(by_rows, by_rows, P("dp", None, "tenant"), P("dp", None, "tenant")),
        check_vma=False,
    )
```
